32 devices in a mesh: rep: 1, dp: 32 (over x, y, z, core).
Axes of the slice: x: 2, y: 2, z: 4, core: 2. Of those that a mesh axis runs over, the one named last changes fastest.
Arguments:
- x: bfloat16 [32, 2048, 896], P(('rep', 'dp'))
- dy: bfloat16 [32, 2048, 896], P(('rep', 'dp'))
- wq: bfloat16 [2, 896, 896], replicated
- wk: bfloat16 [2, 896, 896], replicated
- wv: bfloat16 [2, 896, 896], replicated
- wo: bfloat16 [2, 896, 896], replicated
- w_gate: bfloat16 [2, 896, 3584], replicated
- w_up: bfloat16 [2, 896, 3584], replicated
- w_down: bfloat16 [2, 3584, 896], replicated
- m_wq: float32 [2, 896, 896], P(None, 'dp')
- m_wk: float32 [2, 896, 896], P(None, 'dp')
- m_wv: float32 [2, 896, 896], P(None, 'dp')
- m_wo: float32 [2, 896, 896], P(None, 'dp')
- m_w_gate: float32 [2, 896, 3584], P(None, 'dp')
- m_w_up: float32 [2, 896, 3584], P(None, 'dp')
- m_w_down: float32 [2, 3584, 896], P(None, 'dp')
- v_wq: float32 [2, 896, 896], P(None, 'dp')
- v_wk: float32 [2, 896, 896], P(None, 'dp')
- v_wv: float32 [2, 896, 896], P(None, 'dp')
- v_wo: float32 [2, 896, 896], P(None, 'dp')
- v_w_gate: float32 [2, 896, 3584], P(None, 'dp')
- v_w_up: float32 [2, 896, 3584], P(None, 'dp')
- v_w_down: float32 [2, 3584, 896], P(None, 'dp')
Outputs:
- output 1: bfloat16 [2, 896, 896], P('rep')
- output 2: bfloat16 [2, 896, 896], P('rep')
- output 3: bfloat16 [2, 896, 896], P('rep')
- output 4: bfloat16 [2, 896, 896], P('rep')
- output 5: bfloat16 [2, 896, 3584], P('rep')
- output 6: bfloat16 [2, 896, 3584], P('rep')
- output 7: bfloat16 [2, 3584, 896], P('rep')
- output 8: float32 [2, 896, 896], P('rep', 'dp')
- output 9: float32 [2, 896, 896], P('rep', 'dp')
- output 10: float32 [2, 896, 896], P('rep', 'dp')
- output 11: float32 [2, 896, 896], P('rep', 'dp')
- output 12: float32 [2, 896, 3584], P('rep', 'dp')
- output 13: float32 [2, 896, 3584], P('rep', 'dp')
- output 14: float32 [2, 3584, 896], P('rep', 'dp')
- output 15: float32 [2, 896, 896], P('rep', 'dp')
- output 16: float32 [2, 896, 896], P('rep', 'dp')
- output 17: float32 [2, 896, 896], P('rep', 'dp')
- output 18: float32 [2, 896, 896], P('rep', 'dp')
- output 19: float32 [2, 896, 3584], P('rep', 'dp')
- output 20: float32 [2, 896, 3584], P('rep', 'dp')
- output 21: float32 [2, 3584, 896], P('rep', 'dp')
All inputs are finite; a program needn't handle non-finite values.
Results may differ from the reference program's by a relative error of at most 0.0304.
Values are sent between devices in bfloat16 or wider.
A program may use at most 2 GiB of HBM per device.

```python
import jax
import jax.numpy as jnp
from jax import lax

SEQUENCES = 32
TOKENS = 2048
D = 896
HEADS = 7
KV_HEADS = 7
HEAD = 128
FF = 3584
LAYERS = 2
THETA = 10000
NAMES = ("wq", "wk", "wv", "wo", "w_gate", "w_up", "w_down")
SHAPES = {
    "wq": (LAYERS, D, HEADS * HEAD),
    "wk": (LAYERS, D, KV_HEADS * HEAD),
    "wv": (LAYERS, D, KV_HEADS * HEAD),
    "wo": (LAYERS, HEADS * HEAD, D),
    "w_gate": (LAYERS, D, FF),
    "w_up": (LAYERS, D, FF),
    "w_down": (LAYERS, FF, D),
}


def bump(key, n, height):
    away = (jnp.arange(n, dtype=jnp.int32) - jax.random.randint(key, (), 0, n, jnp.int32)) % n
    return jnp.where(away < n // 8, height, 1.0)


def together(key, own, strength):
    shared = jax.random.normal(key, own.shape[1:], jnp.float32)
    return (own + strength * shared) * lax.rsqrt(1 + strength * strength)


def setup_inputs(seed: int = 0, part: int = 0) -> dict:
    kx, kdy, ka, kb, kz, kf, kh, kl, *keys = jax.random.split(jax.random.key(seed), 8 + 3 * len(NAMES))
    kx, kdy, ka, kb = (jax.random.fold_in(k, part) for k in (kx, kdy, ka, kb))
    kw, km, kv = (keys[i::3] for i in range(3))
    shape = (SEQUENCES, TOKENS, D)
    much_x, much_dy = jax.random.uniform(kz, (2,), jnp.float32, 0.0, 1.0)
    loud = 2.0 ** jax.random.uniform(jax.random.fold_in(kz, 1), (), jnp.float32, -1.0, 2.0)
    layers = 2.0 ** jax.random.uniform(kl, (LAYERS, 1, 1), jnp.float32, -1.0, 1.0)
    times = {"wq": 1.0, "wk": 1.0, "wv": 2.0, "wo": layers, "w_gate": 1.0, "w_up": bump(kh, FF, 4.0), "w_down": layers}
    x = together(ka, jax.random.normal(kx, shape, jnp.float32), much_x) * bump(kf, D, 4.0)
    dy = together(kb, jax.random.normal(kdy, shape, jnp.float32), much_dy)
    drawn = {"x": x.astype(jnp.bfloat16), "dy": (loud * dy * (SEQUENCES * TOKENS) ** -0.5).astype(jnp.bfloat16)}
    for key, name in zip(kw, NAMES, strict=True):
        drawn[name] = (jax.random.normal(key, SHAPES[name], jnp.float32) * SHAPES[name][1] ** -0.5 * times[name]).astype(jnp.bfloat16)
    for key, name in zip(km, NAMES, strict=True):
        drawn[f"m_{name}"] = 0.1 * jax.random.normal(key, SHAPES[name], jnp.float32)
    for key, name in zip(kv, NAMES, strict=True):
        drawn[f"v_{name}"] = jax.random.uniform(key, SHAPES[name], jnp.float32, 0.02, 0.06)
    return drawn


def matmul(a, w):
    return jnp.dot(a, w, preferred_element_type=jnp.float32).astype(jnp.bfloat16)


def normed(h):
    wide = h.astype(jnp.float32)
    scale = lax.rsqrt(jnp.mean(wide**2, -1, keepdims=True) + 1e-6)
    return (wide * scale).astype(jnp.bfloat16)


def turned(t, theta):
    half = t.shape[-1] // 2
    angle = jnp.arange(t.shape[0], dtype=jnp.float32)[:, None] * theta ** (-jnp.arange(half, dtype=jnp.float32) / half)
    cos, sin = jnp.cos(angle)[:, None], jnp.sin(angle)[:, None]
    a, b = t[..., :half].astype(jnp.float32), t[..., half:].astype(jnp.float32)
    return jnp.concatenate([a * cos - b * sin, b * cos + a * sin], -1).astype(jnp.bfloat16)


def seen_by(q, k, v):
    tokens, kv = q.shape[0], k.shape[1]
    q = q.reshape(tokens, kv, -1, q.shape[-1])
    scores = jnp.einsum("tgsd,ugd->gstu", q.astype(jnp.float32), k.astype(jnp.float32)) * q.shape[-1] ** -0.5
    place = jnp.arange(tokens)
    weights = jax.nn.softmax(jnp.where(place[:, None] >= place, scores, -jnp.inf), -1).astype(jnp.bfloat16)
    return jnp.einsum("gstu,ugd->tgsd", weights.astype(jnp.float32), v.astype(jnp.float32)).astype(jnp.bfloat16).reshape(tokens, -1)


def layer(h, w):
    a = normed(h)
    q, k = (turned(matmul(a, w[name]).reshape(h.shape[0], -1, HEAD), THETA) for name in ("wq", "wk"))
    h = h + matmul(seen_by(q, k, matmul(a, w["wv"]).reshape(h.shape[0], -1, HEAD)), w["wo"])
    b = normed(h)
    gate = jnp.dot(b, w["w_gate"], preferred_element_type=jnp.float32)
    up = jnp.dot(b, w["w_up"], preferred_element_type=jnp.float32)
    return h + matmul((jax.nn.silu(gate) * up).astype(jnp.bfloat16), w["w_down"])


def adamw(w, m, v, g):
    m = 0.9 * m + 0.1 * g
    v = 0.95 * v + 0.05 * g * g
    step = m * lax.rsqrt(v + 1e-8) + 0.1 * w
    return (w - 0.02 * step).astype(jnp.bfloat16), m, v


def clipped(gradients, sum_of_squares, count):
    factor = jnp.minimum(1.0, 0.5 * lax.rsqrt(sum_of_squares / count + 1e-30))
    return [g * factor for g in gradients]


def stack(weights, h):
    return lax.scan(lambda h, w: (layer(h, w), None), h, weights)[0]


def reference(x, dy, wq, wk, wv, wo, w_gate, w_up, w_down, m_wq, m_wk, m_wv, m_wo, m_w_gate, m_w_up, m_w_down, v_wq, v_wk, v_wv, v_wo, v_w_gate, v_w_up, v_w_down):
    weights = dict(zip(NAMES, (wq, wk, wv, wo, w_gate, w_up, w_down), strict=True))

    def take(so_far, sequence):
        h, by_y = sequence
        _, back = jax.vjp(stack, weights, h)
        by_weights, by_h = back(by_y)
        return jax.tree.map(lambda total, term: total + term.astype(jnp.float32), so_far, by_weights), by_h

    none_yet = {name: jnp.zeros(w.shape, jnp.float32) for name, w in weights.items()}
    by_weights, by_x = lax.scan(take, none_yet, (x, dy))
    gradients = [by_weights[name].astype(jnp.bfloat16).astype(jnp.float32) for name in NAMES]
    gradients = clipped(gradients, sum(jnp.sum(g * g) for g in gradients), sum(g.size for g in gradients))
    first = (m_wq, m_wk, m_wv, m_wo, m_w_gate, m_w_up, m_w_down)
    second = (v_wq, v_wk, v_wv, v_wo, v_w_gate, v_w_up, v_w_down)
    new = [adamw(weights[name].astype(jnp.float32), m, v, g) for name, m, v, g in zip(NAMES, first, second, gradients, strict=True)]
    return tuple(one[which] for which in range(3) for one in new)
```

```python
import functools

import jax
import jax.numpy as jnp
import numpy as np
from jax import lax
from jax.experimental import pallas as pl
from jax.experimental.pallas import tpu as pltpu
from jax.sharding import Mesh, PartitionSpec as P

NEG = -1e30
HIDDEN = 2 * NEG
LOG2E = 1.4426950408889634
VMEM = 56 * 2**20
HEAD = 128
THETA = 10000
BLOCK = 512
NAMES = ("wq", "wk", "wv", "wo", "w_gate", "w_up", "w_down")


def _dot(a, b, ca, cb):
    return lax.dot_general(a, b, (((ca,), (cb,)), ((), ())), preferred_element_type=jnp.float32)


def _head(n):
    return slice(n * HEAD, (n + 1) * HEAD)


def _causal(keys, queries):
    return lax.broadcasted_iota(jnp.int32, (keys, queries), 1) >= lax.broadcasted_iota(jnp.int32, (keys, queries), 0)


def _project(h_ref, wq_ref, wk_ref, wv_ref, cos_ref, sin_ref, a_ref, q_ref, k_ref, v_ref):
    wide = h_ref[...].astype(jnp.float32)
    scale = lax.rsqrt(jnp.mean(wide * wide, -1, keepdims=True) + 1e-6)
    a = (wide * scale).astype(jnp.bfloat16)
    a_ref[...] = a
    cos, sin = cos_ref[...], sin_ref[...]
    for w_ref, out_ref in ((wq_ref, q_ref), (wk_ref, k_ref)):
        t = _dot(a, w_ref[0], 1, 0).astype(jnp.bfloat16)
        for n in range(t.shape[1] // HEAD):
            x = t[:, _head(n)].astype(jnp.float32)
            out_ref[:, _head(n)] = (x * cos + pltpu.roll(x, HEAD // 2, 1) * sin).astype(jnp.bfloat16)
    v_ref[...] = _dot(a, wv_ref[0], 1, 0).astype(jnp.bfloat16)


def project(h, wq, wk, wv, number, cos, sin):
    tokens, d = h.shape
    block = min(512, tokens)
    rows = lambda width: pl.BlockSpec((block, width), lambda i: (i, 0))
    whole = lambda w: pl.BlockSpec((1,) + w.shape[1:], lambda i: (number, 0, 0))
    widths = (d, wq.shape[2], wk.shape[2], wv.shape[2])
    return pl.pallas_call(
        _project,
        grid=(tokens // block,),
        in_specs=[rows(d), whole(wq), whole(wk), whole(wv), rows(HEAD), rows(HEAD)],
        out_specs=[rows(n) for n in widths],
        out_shape=[jax.ShapeDtypeStruct((tokens, n), jnp.bfloat16) for n in widths],
        compiler_params=pltpu.CompilerParams(dimension_semantics=("parallel",), vmem_limit_bytes=VMEM),
        cost_estimate=pl.CostEstimate(flops=2 * tokens * d * sum(widths[1:]), transcendentals=tokens,
                                      bytes_accessed=2 * (tokens * (d + sum(widths)) + d * sum(widths[1:]))),
        name="project",
    )(h, wq, wk, wv, cos, sin)


def _forward(q_ref, k_ref, v_ref, o_ref, lse_ref, top_s, mix_s, *, heads, scale, size):
    iq = pl.program_id(0)
    e = scale * LOG2E
    top_s[...] = jnp.full_like(top_s, NEG)
    mix_s[...] = jnp.zeros_like(mix_s)
    ones = jnp.ones((8, size), k_ref.dtype)

    def block(j, masked):
        here = pl.ds(pl.multiple_of(j * size, size), size)
        scores = [_dot(k_ref[here, _head(i)], q_ref[:, _head(i)], 1, 1) for i in range(heads)]
        ok = _causal(size, size) if masked else None
        weights, keeps = [], []
        for i, s in enumerate(scores):
            if masked:
                s = jnp.where(ok, s, HIDDEN)
            old = top_s[i : i + 1, :]
            top = jnp.maximum(old, s.max(axis=0, keepdims=True))
            top_s[i : i + 1, :] = top
            weights.append(jnp.exp2((s - top) * e).astype(k_ref.dtype))
            keeps.append(jnp.exp2((old - top) * e))
        for i, (p, keep) in enumerate(zip(weights, keeps)):
            values = jnp.concatenate([v_ref[here, _head(i)].T, ones], axis=0)
            mix_s[i] = mix_s[i] * keep + _dot(values, p, 1, 0)

    lax.fori_loop(0, iq, lambda j, _: block(j, False), None)
    block(iq, True)
    for i in range(heads):
        total = mix_s[i, HEAD : HEAD + 1, :]
        o_ref[:, _head(i)] = (mix_s[i, :HEAD, :] * (1 / total)).T.astype(o_ref.dtype)
        lse_ref[i] = top_s[i : i + 1, :] * scale + jnp.log(total)


def attend(q, k, v):
    tokens, width = q.shape
    heads, size = width // HEAD, min(BLOCK, tokens)
    rows = pl.BlockSpec((size, width), lambda i: (i, 0))
    whole = pl.BlockSpec((tokens, width), lambda i: (0, 0))
    return pl.pallas_call(
        functools.partial(_forward, heads=heads, scale=HEAD**-0.5, size=size),
        grid=(tokens // size,),
        in_specs=[rows, whole, whole],
        out_specs=[rows, pl.BlockSpec((heads, 1, size), lambda i: (0, 0, i))],
        out_shape=[jax.ShapeDtypeStruct((tokens, width), q.dtype), jax.ShapeDtypeStruct((heads, 1, tokens), jnp.float32)],
        scratch_shapes=[pltpu.VMEM((heads, size), jnp.float32), pltpu.VMEM((heads, HEAD + 8, size), jnp.float32)],
        compiler_params=pltpu.CompilerParams(dimension_semantics=("arbitrary",), vmem_limit_bytes=VMEM),
        cost_estimate=pl.CostEstimate(flops=4 * tokens * tokens * width, transcendentals=heads * tokens * tokens, bytes_accessed=8 * tokens * width),
        name="attend",
    )(q, k, v)


def _backward(q_ref, k_ref, v_ref, do_ref, o_ref, lse_ref, cos_ref, sin_ref, dq_ref, dk_ref, dv_ref, dq_s, row_s, *, scale, size):
    tokens, low = q_ref.shape[0], q_ref.dtype
    n, e = tokens // size, scale * LOG2E
    at = lambda s: slice(s * size, (s + 1) * size)
    for s in range(n):
        product = do_ref[at(s), :].astype(jnp.float32) * o_ref[at(s), :].astype(jnp.float32)
        row_s[0:1, at(s)] = product.T.sum(axis=0, keepdims=True)
    row_s[1:2, :] = lse_ref[0] * LOG2E
    ok = _causal(size, size)

    def back(g, s):
        g = g.astype(low).astype(jnp.float32)
        return (g * cos_ref[at(s), :] - pltpu.roll(g, HEAD // 2, 1) * sin_ref[at(s), :]).astype(low)

    for j in range(n):
        key, value = k_ref[at(j), :], v_ref[at(j), :]
        turned_key = key.T
        scores = [_dot(key, q_ref[at(s), :], 1, 1) for s in range(j, n)]
        dps = [_dot(value, do_ref[at(s), :], 1, 1) for s in range(j, n)]
        dk = dv = None
        for s, score, dp in zip(range(j, n), scores, dps):
            p = jnp.exp2(score * e - row_s[1:2, at(s)])
            if s == j:
                p = jnp.where(ok, p, 0.0)
            ds = (p * (dp - row_s[0:1, at(s)])).astype(low)
            more_dv, more_dk, more_dq = _dot(p.astype(low), do_ref[at(s), :], 1, 0), _dot(ds, q_ref[at(s), :], 1, 0), _dot(turned_key, ds, 1, 0)
            dv = more_dv if dv is None else dv + more_dv
            dk = more_dk if dk is None else dk + more_dk
            dq_s[:, at(s)] = more_dq if j == 0 else dq_s[:, at(s)] + more_dq
        dv_ref[at(j), :] = dv.astype(low)
        dk_ref[at(j), :] = back(dk * scale, j)
    for s in range(n):
        dq_ref[at(s), :] = back((dq_s[:, at(s)] * scale).T, s)


def attend_bwd(q, k, v, d_out, out, lse, cos, sin):
    tokens, width = q.shape
    heads, size = width // HEAD, min(BLOCK, tokens)
    column = pl.BlockSpec((tokens, HEAD), lambda i: (0, i))
    table = pl.BlockSpec((tokens, HEAD), lambda i: (0, 0))
    return pl.pallas_call(
        functools.partial(_backward, scale=HEAD**-0.5, size=size),
        grid=(heads,),
        in_specs=[column] * 5 + [pl.BlockSpec((1, 1, tokens), lambda i: (i, 0, 0)), table, table],
        out_specs=[column] * 3,
        out_shape=[jax.ShapeDtypeStruct((tokens, width), q.dtype)] * 3,
        scratch_shapes=[pltpu.VMEM((HEAD, tokens), jnp.float32), pltpu.VMEM((8, tokens), jnp.float32)],
        compiler_params=pltpu.CompilerParams(dimension_semantics=("parallel",), vmem_limit_bytes=VMEM),
        cost_estimate=pl.CostEstimate(flops=10 * tokens * tokens * width, transcendentals=heads * tokens * tokens, bytes_accessed=16 * tokens * width),
        name="attend_bwd",
    )(q, k, v, d_out, out, lse, cos, sin)


def _unpack(rows_ref, *outs):
    start = 0
    for out in outs:
        count, n = rows_ref.shape[2], out.shape[2]
        for run in range(0, out.shape[1], count):
            out[0, run : run + count, :] = rows_ref[0, 0, :, start : start + n]
            start += n


def unpack(rows, weights):
    chips, layers = rows.shape[:2]
    return pl.pallas_call(
        _unpack,
        grid=(layers, chips),
        in_specs=[pl.BlockSpec((1, 1, *rows.shape[2:]), lambda i, j: (j, i, 0, 0))],
        out_specs=[pl.BlockSpec((1, w.shape[1] // chips, w.shape[2]), lambda i, j: (i, j, 0)) for w in weights],
        out_shape=[jax.ShapeDtypeStruct(w.shape, w.dtype) for w in weights],
        compiler_params=pltpu.CompilerParams(dimension_semantics=("parallel", "parallel"), vmem_limit_bytes=32 * 2**20),
        cost_estimate=pl.CostEstimate(flops=0, transcendentals=0, bytes_accessed=4 * rows.size),
        name="unpack",
    )(rows)


def matmul(a, w):
    return jnp.dot(a, w, preferred_element_type=jnp.float32).astype(jnp.bfloat16)


def normed(h):
    wide = h.astype(jnp.float32)
    scale = lax.rsqrt(jnp.mean(wide**2, -1, keepdims=True) + 1e-6)
    return (wide * scale).astype(jnp.bfloat16)


def turns(tokens):
    half = HEAD // 2
    angle = np.arange(tokens)[:, None] * float(THETA) ** (-np.arange(half) / half)
    cos, sin = np.cos(angle), np.sin(angle)
    return (jnp.asarray(np.concatenate(two, -1), jnp.float32) for two in ((cos, cos), (-sin, sin)))


def gated(gate, up):
    return (jax.nn.silu(gate) * up).astype(jnp.bfloat16)


def spread(rows, devices):
    block = rows // devices
    padded = -(-block // 16) * 16
    place = np.arange(rows)
    one = np.zeros((rows, devices * padded), np.float32)
    one[place, place // block * padded + place % block] = 1
    return jnp.asarray(one, jnp.bfloat16)


def product(a, b):
    return _dot(a, b, 0, 0).astype(jnp.bfloat16)


def adamw(w, m, v, g):
    m = 0.9 * m + 0.1 * g
    v = 0.95 * v + 0.05 * g * g
    step = m * lax.rsqrt(v + 1e-8) + 0.1 * w
    return (w - 0.02 * step).astype(jnp.bfloat16), m, v


MESH = pl.DeviceIdType.MESH


def _place():
    return {name: lax.axis_index(name) for name in ("x", "y", "z", "core")}


def _partners(at):
    high, low = at["z"] // 2, at["z"] % 2
    return [{"core": 1 - at["core"]}, {"x": 1 - at["x"]}, {"y": 1 - at["y"]}, {"z": 2 * high + 1 - low}, {"z": 2 * (1 - high) + low}]


def _meet(partners):
    barrier = pltpu.get_barrier_semaphore()
    for partner in partners:
        pl.semaphore_signal(barrier, inc=1, device_id=partner, device_id_type=MESH)
    pl.semaphore_wait(barrier, len(partners))


def _scatter(*refs, count):
    given, outs, rest = refs[:count], refs[count : 2 * count], refs[2 * count :]
    own, got = rest[:count], [rest[i * count : (i + 1) * count] for i in range(1, 6)]
    load_sem, send_sem, recv_sem = rest[6 * count :]
    at = _place()
    x, y, high, low, core = at["x"], at["y"], at["z"] // 2, at["z"] % 2, at["core"]
    partners = _partners(at)
    _meet(partners)

    def remote(step, k, source, partner):
        return pltpu.make_async_remote_copy(src_ref=source, dst_ref=got[step][k], send_sem=send_sem.at[step, k], recv_sem=recv_sem.at[step, k],
                                            device_id=partner, device_id_type=MESH)

    flights = [[None] * count for _ in range(5)]
    loads = []
    for k in range(count):
        flights[0][k] = remote(0, k, given[k].at[:, :, :, :, 1 - core], partners[0])
        flights[0][k].start()
        loads.append(pltpu.make_async_copy(given[k].at[:, :, :, :, core], own[k], load_sem.at[k]))
        loads[k].start()

    def total(k, steps, i, j, a, b):
        t = own[k][i, j, a, b].astype(jnp.float32) + got[0][k][i, j, a, b].astype(jnp.float32)
        places = [(j, a, b) if k % 2 == 0 else (i, a, b), (a, b), (a,), ()]
        for step in range(1, steps):
            place = places[step - 1]
            t = t + got[step][k][place if place else ...].astype(jnp.float32)
        return t

    def send(step, k):
        along_x = (k % 2 == 0) == (step == 1)
        if step == 1:
            @pl.loop(0, 8)
            def _(n):
                m, a, b = n // 4, n // 2 % 2, n % 2
                i, j = (1 - x, m) if along_x else (m, 1 - y)
                own[k][i, j, a, b] = total(k, 1, i, j, a, b).astype(jnp.bfloat16)

            source = own[k].at[1 - x] if along_x else own[k].at[:, 1 - y]
            partner = partners[1] if along_x else partners[2]
        elif step == 2:
            i, j = (1 - x, y) if along_x else (x, 1 - y)

            @pl.loop(0, 4)
            def _(n):
                a, b = n // 2, n % 2
                own[k][i, j, a, b] = total(k, 2, i, j, a, b).astype(jnp.bfloat16)

            source, partner = own[k].at[i, j], partners[1] if along_x else partners[2]
        elif step == 3:
            @pl.loop(0, 2)
            def _(a):
                own[k][x, y, a, 1 - low] = total(k, 3, x, y, a, 1 - low).astype(jnp.bfloat16)

            source, partner = own[k].at[x, y, :, 1 - low], partners[3]
        else:
            own[k][x, y, 1 - high, low] = total(k, 4, x, y, 1 - high, low).astype(jnp.bfloat16)
            source, partner = own[k].at[x, y, 1 - high, low], partners[4]
        flights[step][k] = remote(step, k, source, partner)
        flights[step][k].start()

    for turn in range(count + 5):
        for k in range(count):
            step = turn - k
            if step == 0:
                loads[k].wait()
                flights[0][k].wait()
                send(1, k)
            elif 1 <= step <= 3:
                flights[step][k].wait()
                send(step + 1, k)
            elif step == 4:
                flights[4][k].wait()
                outs[k][...] = total(k, 5, x, y, high, low).astype(jnp.bfloat16)


def scatter_sum(gradients):
    count = len(gradients)
    given = [g.reshape(2, 2, 2, 2, 2, g.shape[0] // 32, g.shape[1]) for g in gradients]
    shapes = [g.shape[5:] for g in given]
    scratch = [pltpu.VMEM(lead + s, jnp.bfloat16) for lead in ((2, 2, 2, 2), (2, 2, 2, 2), (2, 2, 2), (2, 2), (2,), ()) for s in shapes]
    size = sum(g.size for g in gradients)
    return pl.pallas_call(
        functools.partial(_scatter, count=count),
        in_specs=[pl.BlockSpec(memory_space=pl.ANY)] * count,
        out_specs=[pl.BlockSpec(memory_space=pltpu.VMEM)] * count,
        out_shape=[jax.ShapeDtypeStruct(s, jnp.bfloat16) for s in shapes],
        scratch_shapes=scratch + [pltpu.SemaphoreType.DMA((count,)), pltpu.SemaphoreType.DMA((5, count)), pltpu.SemaphoreType.DMA((5, count))],
        compiler_params=pltpu.CompilerParams(collective_id=0, has_side_effects=True, vmem_limit_bytes=62 * 2**20),
        cost_estimate=pl.CostEstimate(flops=2 * size, transcendentals=0, bytes_accessed=4 * size),
        name="scatter_sum",
    )(*given)


def _total(mine_ref, out_ref, sent, got, send_sem, recv_sem):
    partners = _partners(_place())
    _meet(partners)
    t = mine_ref[...]
    for step, partner in enumerate(partners):
        sent[step] = t
        copy = pltpu.make_async_remote_copy(src_ref=sent.at[step], dst_ref=got.at[step], send_sem=send_sem.at[step], recv_sem=recv_sem.at[step],
                                            device_id=partner, device_id_type=MESH)
        copy.start()
        copy.wait()
        t = t + got[step]
    out_ref[...] = t


def group_sum(t):
    return pl.pallas_call(
        _total,
        in_specs=[pl.BlockSpec(memory_space=pltpu.VMEM)],
        out_specs=pl.BlockSpec(memory_space=pltpu.VMEM),
        out_shape=jax.ShapeDtypeStruct(t.shape, t.dtype),
        scratch_shapes=[pltpu.VMEM((5, *t.shape), t.dtype), pltpu.VMEM((5, *t.shape), t.dtype), pltpu.SemaphoreType.DMA((5,)), pltpu.SemaphoreType.DMA((5,))],
        compiler_params=pltpu.CompilerParams(collective_id=1, has_side_effects=True, vmem_limit_bytes=2**20),
        name="group_sum",
    )(t)


def solution(mesh):
    z = mesh.shape["dp"] // 8
    inner = Mesh(mesh.devices.reshape(2, 2, z, 2), ("x", "y", "z", "core"))
    chips = ("x", "y", "z")
    everyone = chips + ("core",)
    swap = [(0, 1), (1, 0)]

    def step(x, dy, *arrays):
        weights, m, v = (arrays[i : i + 7] for i in (0, 7, 14))
        wq, wk, wv, wo, w_gate, w_up, w_down = weights
        layers, devices = wq.shape[0], lax.psum(1, everyone)
        h = x[0]
        cos, sin = turns(h.shape[0])
        fill = spread(h.shape[1], devices)
        kept = []
        for number in range(layers):
            a, q, k, vv = project(h, wq, wk, wv, number, cos, sin)
            out, lse = attend(q, k, vv)
            mid = h + matmul(out, wo[number])
            b = normed(mid)
            gate = jnp.dot(b, w_gate[number], preferred_element_type=jnp.float32)
            up = jnp.dot(b, w_up[number], preferred_element_type=jnp.float32)
            kept.append((h, a, q, k, vv, out, lse, mid, b, gate, up))
            h = mid + matmul(gated(gate, up), w_down[number])

        def scattered(gradient):
            return lax.psum_scatter(gradient, everyone, scatter_dimension=0, tiled=True)

        together = lax.optimization_barrier
        waiting, sums = [], []

        def turn(*others):
            if waiting:
                done, gradient, *others = together((sums[-1:], waiting.pop(0), *others))
                sums[-1:] = done
                sums.append(scattered(gradient))
            return others

        by_h, mine = dy[0], [None] * layers
        for number in reversed(range(layers)):
            last = number == layers - 1
            h_in, a, q, k, vv, out, lse, mid, b, gate, up = kept[number]
            by_act = matmul(by_h, w_down[number].T)
            act, back = jax.vjp(gated, gate, up)
            by_gate, by_up = (t.astype(jnp.bfloat16) for t in back(by_act))
            d_down = product(act, by_h)
            if last:
                waiting.append(d_down)
            by_gate, by_up = turn(by_gate, by_up)
            b = matmul(b, fill)
            d_gate, d_up = product(b, by_gate), product(b, by_up)
            by_gate, by_up, d_gate, d_up = together((by_gate, by_up, d_gate, d_up))
            if last:
                waiting += [d_gate, d_up]
            by_b = matmul(by_gate, w_gate[number].T) + matmul(by_up, w_up[number].T)
            by_mid = by_h + jax.vjp(normed, mid)[1](by_b)[0]
            d_o = product(matmul(out, fill), by_mid)
            by_out = matmul(by_mid, wo[number].T)
            by_out, d_o = together((by_out, d_o))
            if last:
                (by_out,) = turn(by_out)
            dq, dk, dv = attend_bwd(q, k, vv, by_out, out, lse, cos, sin)
            a = matmul(a, fill)
            d_qkvo = jnp.concatenate([product(a, dq), product(a, dk), product(a, dv), d_o], axis=1)
            if number:
                dq, dk, dv, d_qkvo = together((dq, dk, dv, d_qkvo))
                by_a = matmul(dq, wq[number].T) + matmul(dk, wk[number].T) + matmul(dv, wv[number].T)
                by_h = by_mid + jax.vjp(normed, h_in)[1](by_a)[0]
            if last:
                waiting.append(d_qkvo)
                (by_h,) = turn(by_h)
                late = sums
            else:
                early = scatter_sum([d_gate, d_up, d_down, d_qkvo])
        d, rows = h.shape[1], h.shape[1] // devices

        def named(down, g_gate, g_up, qkvo):
            return [qkvo[:rows, i * d : (i + 1) * d] for i in range(4)] + [g_gate[:rows], g_up[:rows], down]

        mine = [named(early[2], early[0], early[1], early[3]), named(*late)]
        gradients = [jnp.stack([mine[number][i] for number in range(layers)]).astype(jnp.float32) for i in range(7)]
        squares = group_sum(jnp.broadcast_to(sum(jnp.sum(g * g) for g in gradients), (8, 128)))[0, 0]
        factor = jnp.minimum(1.0, 0.5 * lax.rsqrt(squares / (devices * sum(g.size for g in gradients)) + 1e-30))
        me, core = lax.axis_index(everyone), lax.axis_index("core")
        new = []
        for w, one, two, g in zip(weights, m, v, gradients, strict=True):
            own = lax.dynamic_slice_in_dim(w, me * one.shape[1], one.shape[1], 1).astype(jnp.float32)
            new.append(adamw(own, one, two, g * factor))

        zero = core == 0

        def paired(t):
            got = lax.ppermute(jnp.where(zero, t[1], t[0]), "core", swap)
            return jnp.where(zero, jnp.concatenate([t[0], got]), jnp.concatenate([got, t[1]]))

        pack = paired(jnp.concatenate([one[0] for one in new[:6]], axis=2))
        tall = paired(new[6][0])
        runs = tall.shape[0] // pack.shape[0]
        pack = jnp.concatenate([pack, *jnp.split(tall, runs)], axis=1)
        all_rows = lax.all_gather(pack, everyone, axis=0).reshape(devices // 2, 2, *pack.shape)
        whole = unpack(all_rows, weights)
        return (*whole, *(one[1] for one in new), *(one[2] for one in new))

    states, all_of, cut = P(everyone, None, None), P(None, None, None), P(None, everyone, None)
    return jax.shard_map(
        step,
        mesh=inner,
        in_specs=(states, states) + (all_of,) * 7 + (cut,) * 14,
        out_specs=(all_of,) * 7 + (cut,) * 14,
        check_vma=False,
    )
```
